32 devices in a mesh: ep: 8 (over y, x, core), tp: 4 (over z).
Axes of the slice: x: 2, y: 2, z: 4, core: 2. Of those that a mesh axis runs over, the one named last changes fastest.
Arguments:
- tokens: bfloat16 [512, 7168], P('ep'), may hold values from -6 to 6
- gate_scores: float32 [512, 8], P('ep'), may hold values from 0.1 to 1
- expert_ids: int32 [512, 8], P('ep'), may hold values from 0 to 15, all different within a row; in each aligned block of 64 rows (0 to 63, 64 to 127, ...) at most 48 rows name the same one
- gate_weight: bfloat16 [16, 7168, 2048], P('ep', None, 'tp'), may hold values from -0.0625 to 0.0625
- up_weight: bfloat16 [16, 7168, 2048], P('ep', None, 'tp'), may hold values from -0.0625 to 0.0625
- down_weight: bfloat16 [16, 2048, 7168], P('ep', 'tp'), may hold values from -0.125 to 0.125
Outputs:
- mixed: bfloat16 [512, 7168], P('ep', 'tp')
The draws below stay inside these ranges and needn't reach their ends.
Inputs may be any that keep to these rules, and one draw needn't show every extreme that they name: `expert_ids`: each row names 8 different experts. Among the tokens of one group, no expert is named by more than 48 tokens, and in every draw some expert is named by exactly 48 of them.
All inputs are finite; a program needn't handle non-finite values.
Results may differ from the reference program's by a relative error of at most 0.02.
Values may be sent and summed in bfloat16 or wider, within the bound.
No kernel may reach another device: no remote copies, remote signals or barrier semaphores. Data moves between devices by JAX's collectives and lax.ppermute only.
A program may use at most 192 MiB of HBM per device.

```python
import math
import jax
import jax.numpy as jnp
import numpy as np
from jax import lax

D = 7168
FF = 2048
TOPK = 8
TOK_DEV = 64
EXPERTS = 16
CAP = 48
TOKENS = 512
N_EP = 8
N_TP = 4


def block_levels(own_key, dims, pieces, smallest, top_value):
    gain = 1.0
    for dim, shards_of in pieces:
        draws = jax.random.uniform(jax.random.fold_in(jax.random.fold_in(own_key, 6), dim), (shards_of,), jnp.float32, smallest / len(pieces), top_value / len(pieces))
        gain = gain * jnp.repeat(jnp.exp(draws), dims[dim] // shards_of).reshape((-1,) + (1,) * (len(dims) - 1 - dim))
    return gain


def shared_out(own_key, own, number, rows, amount, top, reach, slope):
    order = jax.random.permutation(own_key, amount)
    crowded, usual = load_shares(amount, rows * top, reach, slope, True), load_shares(amount, rows * top, reach, slope, False)
    places = jnp.arange(amount)

    def named(sizes, turn):
        used = int((sizes > 0).sum())
        fixed = max(1, used // 4)
        shifted = fixed + (places - fixed + turn * (used - fixed)) % max(1, amount - fixed)
        return jnp.zeros((amount,), jnp.int32).at[order[jnp.where(places < fixed, places, shifted)]].set(jnp.asarray(sizes, jnp.int32))

    sizes = jnp.where(number % 4 == 0, named(crowded, number // 4), named(usual, number - number // 4 - 1))
    mixed = jax.random.permutation(jax.random.fold_in(own, 3), amount)
    source_of, receiver = mixed[0:amount // 2 * 2:2], mixed[1:amount // 2 * 2:2]
    slack = jnp.minimum(sizes[source_of] - 1, reach - sizes[receiver]) // 2
    slack = jnp.where((source_of == order[0]) | (receiver == order[0]) | (sizes[receiver] == 0), 0, jnp.maximum(slack, 0))
    shifted = jax.random.randint(jax.random.fold_in(own, 4), (amount // 2,), 0, 1 << 20) % (slack + 1)
    sizes = sizes.at[source_of].add(-shifted).at[receiver].add(shifted)
    labels = jnp.searchsorted(jnp.cumsum(sizes), jnp.arange(rows * top), side="right").astype(jnp.int32)
    table = labels.reshape(top, rows).T
    table = table[jax.random.permutation(jax.random.fold_in(own, 1), rows)]
    turn = jax.random.randint(jax.random.fold_in(own, 2), (rows, 1), 0, top)
    return jnp.take_along_axis(table, (jnp.arange(top)[None, :] + turn) % top, axis=1)


def load_shares(count, total, bound, slope, full):
    weights = [(1 << 20) // math.isqrt(grade ** slope) + 1 for grade in range(1, count + 1)]
    largest = bound if full else min(bound, max(-(-total // count), total * weights[0] // sum(weights)))
    least = 1 if total - largest >= count - 1 else 0
    counts, surplus = [largest] + [least] * (count - 1), total - largest - least * (count - 1)
    while surplus > 0:
        free = [i for i in range(1, count) if counts[i] < largest] or [i for i in range(1, count) if counts[i] < bound]
        mass, remaining = sum([weights[i] for i in free]), surplus
        for i in free:
            more = min(bound - counts[i], max(1, remaining * weights[i] // mass), surplus)
            counts[i] = counts[i] + more
            surplus = surplus - more
    return np.array(counts)


def scatter_about(rng, dims, scale, most, cuts=(), kind=jnp.bfloat16):
    drawn = jax.random.normal(rng, dims, jnp.float32) * scale
    if len(cuts) > 0:
        drawn = block_levels(rng, dims, cuts, -0.22, 0.18) * drawn
    return jnp.clip(drawn, min=-most, max=most).astype(kind)


def setup_inputs(seed: int = 0) -> dict:
    splits = jax.random.split(jax.random.key(seed), 7)
    tokens = scatter_about(splits[0], (TOKENS, D), 1.0, 6.0, ((0, 8),))
    gate_scores = jnp.clip(jnp.exp(math.log(1.0) - 2.3025851 * jax.random.uniform(splits[1], (TOKENS, TOPK), jnp.float32) ** block_levels(splits[1], (TOKENS, TOPK), ((0, 8),), -0.2, 0.2)), 0.1, 1.0)
    expert_ids_keys = jax.random.split(jax.random.fold_in(splits[2], 1), TOKENS // TOK_DEV)
    expert_ids_turns = jax.random.permutation(jax.random.fold_in(splits[2], 3), TOKENS // TOK_DEV)
    expert_ids = jax.vmap(lambda own, number: shared_out(jax.random.fold_in(splits[2], 2), own, number, TOK_DEV, EXPERTS, TOPK, CAP, 2))(expert_ids_keys, expert_ids_turns).reshape((TOKENS, TOPK))
    gate_weight = scatter_about(splits[3], (EXPERTS, D, FF), D ** -0.5, 0.0625, ((0, 8), (2, 4)))
    up_weight = scatter_about(splits[4], (EXPERTS, D, FF), D ** -0.5, 0.0625, ((0, 8), (2, 4)))
    down_weight = scatter_about(splits[5], (EXPERTS, FF, D), FF ** -0.5, 0.125, ((0, 8), (1, 4)))
    return dict(tokens=tokens, gate_scores=gate_scores, expert_ids=expert_ids, gate_weight=gate_weight, up_weight=up_weight, down_weight=down_weight)


def tables(ids_group):
    expert_range = jnp.arange(EXPERTS).astype(jnp.int32)
    picked = jnp.sum((ids_group[:, :, None] == expert_range[None, None, :]).astype(jnp.int32), axis=1)
    rank = jnp.cumsum(picked, axis=0) - picked
    slot = jnp.take_along_axis(rank, ids_group, axis=1)
    token_range = jnp.arange(TOK_DEV).astype(jnp.int32)
    slot_range = jnp.arange(CAP).astype(jnp.int32)
    hits = (rank.T[:, None, :] == slot_range[None, :, None]) & (picked.T[:, None, :] > 0)
    found = jnp.any(hits, axis=2)
    index = jnp.where(found, jnp.sum(hits.astype(jnp.int32) * token_range[None, None, :], axis=2), TOK_DEV)
    return slot, index.astype(jnp.int32)


def reference(tokens, gate_scores, expert_ids, gate_weight, up_weight, down_weight):
    ids_grouped = expert_ids.reshape(N_EP, TOK_DEV, TOPK)
    slot, index = jax.vmap(tables)(ids_grouped)
    padded = jnp.concatenate([tokens.reshape(N_EP, TOK_DEV, D), jnp.zeros((N_EP, 1, D), jnp.bfloat16)], axis=1)
    width_part = FF // N_TP

    def expert_out(expert):
        chosen = jax.vmap(lambda block, where: block[where])(padded, index[:, expert])
        chosen = chosen.reshape(N_EP * CAP, D)
        gate = jnp.dot(chosen, gate_weight[expert], preferred_element_type=jnp.float32)
        upper = jnp.dot(chosen, up_weight[expert], preferred_element_type=jnp.float32)
        hidden = (jax.nn.silu(gate) * upper).astype(jnp.bfloat16)
        hidden_parts = hidden.reshape(N_EP * CAP, N_TP, width_part).astype(jnp.float32)
        down_parts = down_weight[expert].reshape(N_TP, width_part, D).astype(jnp.float32)
        partial_value = jnp.einsum("rjf,jfd->jrd", hidden_parts, down_parts).astype(jnp.bfloat16)
        partial_value = lax.optimization_barrier(partial_value)
        summed = jnp.sum(partial_value.astype(jnp.float32), axis=0)
        return summed.astype(jnp.bfloat16).reshape(N_EP, CAP, D)

    outputs = lax.map(expert_out, jnp.arange(EXPERTS).astype(jnp.int32))
    groups = (jnp.arange(TOKENS).astype(jnp.int32) // TOK_DEV)[:, None] * jnp.ones((1, TOPK), jnp.int32)
    flat_slot = slot.reshape(TOKENS, TOPK)
    picked_rows = outputs[expert_ids, groups, flat_slot]
    weights = 2.5 * gate_scores / jnp.sum(gate_scores, axis=1, keepdims=True)
    mixed = jnp.einsum("tk,tkd->td", weights, picked_rows.astype(jnp.float32))
    return mixed.astype(jnp.bfloat16)
```

```python
import functools
import jax
import jax.numpy as jnp
from jax import lax
from jax.experimental import pallas as pl
from jax.experimental.pallas import tpu as pltpu
from jax.sharding import PartitionSpec as P

CHUNKS = 2


def tile_of(size, want):
    tile = min(size, want)
    while size % tile:
        tile -= 128
    return tile


def expert_kernel(counts, groups, k_steps, d_steps, *refs):
    pieces = refs[: len(counts)]
    scale, gate_w, up_w, down_w = refs[len(counts) : len(counts) + 4]
    outs = refs[len(counts) + 4 : len(counts) + 4 + len(groups)]
    gate_acc, up_acc, hidden = refs[len(counts) + 4 + len(groups) :]
    step = pl.program_id(0)
    exp_local, _, ff = gate_w.shape

    @pl.when(step < k_steps)
    def _():
        rows = jnp.concatenate([p[...] for p in pieces], axis=0)
        for e in range(exp_local):
            for acc, weight in ((gate_acc, gate_w), (up_acc, up_w)):
                product = jnp.dot(rows, weight[e], preferred_element_type=jnp.float32)

                @pl.when(step == 0)
                def _():
                    acc[e] = product

                @pl.when(step > 0)
                def _():
                    acc[e] += product

    @pl.when(step == k_steps - 1)
    def _():
        for e in range(exp_local):
            gate = gate_acc[e]
            value = gate / (1.0 + jnp.exp(-gate)) * up_acc[e] * scale[:, e : e + 1]
            hidden[:, e * ff : (e + 1) * ff] = value.astype(jnp.bfloat16)

    @pl.when(step >= k_steps)
    def _():
        down = down_w[...].reshape(exp_local * ff, down_w.shape[2])
        first = 0
        for out, rows_of in zip(outs, groups):
            here = hidden[first : first + rows_of, :]
            out[...] = jnp.dot(here, down, preferred_element_type=jnp.float32).astype(out.dtype)
            first += rows_of


def experts(pieces, groups, scale, gate_weight, up_weight, down_weight):
    exp_local, width, ff = gate_weight.shape
    counts = [p.shape[0] for p in pieces]
    total = sum(counts)
    k_tile, d_tile = tile_of(width, 1024), tile_of(width, 1024)
    k_steps, d_steps = width // k_tile, width // d_tile
    at_k = lambda s: jnp.minimum(s, k_steps - 1)
    at_d = lambda s: jnp.maximum(s - k_steps, 0)
    in_specs = [pl.BlockSpec((c, k_tile), lambda s: (0, at_k(s))) for c in counts]
    in_specs += [
        pl.BlockSpec((total, exp_local), lambda s: (0, 0)),
        pl.BlockSpec((exp_local, k_tile, ff), lambda s: (0, at_k(s), 0)),
        pl.BlockSpec((exp_local, k_tile, ff), lambda s: (0, at_k(s), 0)),
        pl.BlockSpec((exp_local, ff, d_tile), lambda s: (0, 0, at_d(s))),
    ]
    weight_bytes = 2 * 3 * exp_local * width * ff
    return pl.pallas_call(
        functools.partial(expert_kernel, counts, groups, k_steps, d_steps),
        grid=(k_steps + d_steps,),
        in_specs=in_specs,
        out_specs=[pl.BlockSpec((g, d_tile), lambda s: (0, at_d(s))) for g in groups],
        out_shape=[jax.ShapeDtypeStruct((g, width), jnp.bfloat16) for g in groups],
        scratch_shapes=[
            pltpu.VMEM((exp_local, total, ff), jnp.float32),
            pltpu.VMEM((exp_local, total, ff), jnp.float32),
            pltpu.VMEM((total, exp_local * ff), jnp.bfloat16),
        ],
        compiler_params=pltpu.CompilerParams(
            dimension_semantics=("arbitrary",), vmem_limit_bytes=40 * 1024 * 1024
        ),
        cost_estimate=pl.CostEstimate(
            flops=6 * total * exp_local * width * ff,
            bytes_accessed=weight_bytes + 4 * total * width,
            transcendentals=total * exp_local * ff,
        ),
        name="experts",
    )(*pieces, scale, gate_weight, up_weight, down_weight)


def combine_table(gate_scores, expert_ids, experts_all):
    weights = 2.5 * gate_scores / jnp.sum(gate_scores, axis=1, keepdims=True)
    chosen = expert_ids[:, :, None] == jnp.arange(experts_all)[None, None, :]
    return jnp.sum(jnp.where(chosen, weights[:, :, None], 0.0), axis=1)


def add(a, b):
    return (a.astype(jnp.float32) + b.astype(jnp.float32)).astype(jnp.bfloat16)


def share_out(rows):
    n_tp = lax.axis_size("tp")
    me = lax.axis_index("tp")
    share = rows.shape[1] // n_tp
    take = lambda at: lax.dynamic_slice_in_dim(rows, at * share, share, axis=1)
    total = take(me).astype(jnp.float32)
    parts = []
    for k in reversed(range(1, n_tp)):
        perm = [(i, (i + k) % n_tp) for i in range(n_tp)]
        parts.append(lax.ppermute(take(lax.rem(me + k, n_tp)), "tp", perm))
    for part in parts:
        total = total + part.astype(jnp.float32)
    return total.astype(jnp.bfloat16)


def local_by_pairs(tokens, gate_scores, expert_ids, gate_weight, up_weight, down_weight):
    n_ep = lax.axis_size("ep")
    exp_local = gate_weight.shape[0]
    tok = tokens.shape[0]
    me = lax.axis_index("ep")
    pair = [(i, i ^ 1) for i in range(n_ep)]
    side = [(i, i ^ (4 if i % 2 else 2)) for i in range(n_ep)]
    cross = [(i, i ^ (2 if i % 2 else 4)) for i in range(n_ep)]
    send = lambda x, perm: lax.ppermute(x, "ep", perm)

    partner = send(tokens, pair)
    table = combine_table(gate_scores, expert_ids, exp_local * n_ep)
    table = lax.all_gather(table, "ep", axis=0)
    odd = lax.rem(me, 2)
    near, far = 2 + 2 * odd, 4 - 2 * odd
    sources = jnp.stack([far + 1, far, me * 0 + 7, near, near + 1, me * 0 + 6, me * 0, me * 0 + 1])
    table = lax.dynamic_slice_in_dim(table, me * exp_local, exp_local, axis=2)
    table = table[jnp.bitwise_xor(me, sources)]

    rows = tok // CHUNKS
    sent = []
    for j in range(CHUNKS):
        own, mate = (t[j * rows : (j + 1) * rows] for t in (tokens, partner))
        block = send(jnp.concatenate([own, mate], axis=0), side)
        sent.append((own, mate, block))
    results = []
    for j, (own, mate, block) in enumerate(sent):
        corner = send(block[:rows], cross)
        block_mate = send(block, pair)
        corner_mate = send(corner, pair)
        scale = table[:, j * rows : (j + 1) * rows].reshape(n_ep * rows, exp_local)
        away, kept_block, kept_corner, here, here_mate = experts(
            [block_mate, corner_mate, block, corner, own, mate],
            [3 * rows, 2 * rows, rows, rows, rows],
            scale, gate_weight, up_weight, down_weight,
        )
        away = send(away, pair)
        corner = send(add(kept_corner, away[2 * rows :]), cross)
        block_low = add(add(kept_block[:rows], away[:rows]), corner)
        block_high = add(kept_block[rows:], away[rows : 2 * rows])
        block = send(jnp.concatenate([block_low, block_high], axis=0), side)
        mate = send(add(here_mate, block[rows:]), pair)
        results.append(share_out(add(add(here, block[:rows]), mate)))
    return jnp.concatenate(results, axis=0)


def local(tokens, gate_scores, expert_ids, gate_weight, up_weight, down_weight):
    n_ep = lax.axis_size("ep")
    exp_local = gate_weight.shape[0]
    me = lax.axis_index("ep")
    table = combine_table(gate_scores, expert_ids, exp_local * n_ep)
    table = lax.all_gather(table, "ep", axis=0, tiled=True)
    table = lax.dynamic_slice_in_dim(table, me * exp_local, exp_local, axis=1)
    rows = lax.all_gather(tokens, "ep", axis=0, tiled=True)
    (partial,) = experts(
        [rows], [rows.shape[0]], table, gate_weight, up_weight, down_weight
    )
    summed = lax.psum_scatter(partial, "ep", scatter_dimension=0, tiled=True)
    return lax.psum_scatter(summed, "tp", scatter_dimension=1, tiled=True)


def solution(mesh):
    placed = (
        P("ep", None),
        P("ep", None),
        P("ep", None),
        P("ep", None, "tp"),
        P("ep", None, "tp"),
        P("ep", "tp", None),
    )
    body = local_by_pairs if mesh.shape["ep"] == 8 else local
    return jax.shard_map(
        body, mesh=mesh, in_specs=placed, out_specs=P("ep", "tp"), check_vma=False
    )
```
